32 devices in a mesh: band: 8 (over y, x, core), gblk: 4 (over z).
Axes of the slice: x: 2, y: 2, z: 4, core: 2. Of those that a mesh axis runs over, the one named last changes fastest.
Arguments:
- eps_inv: bfloat16 [2, 2, 8, 4, 512, 16384], P(None, None, None, 'gblk', None, 'band'), may hold values from -6 to 6
- pair_elements: bfloat16 [2, 1, 16, 16384], P(None, None, 'band'), may hold values from -0.046875 to 0.046875
Outputs:
- sigma_terms: float32 [2, 2, 1, 16], P(None, None, None, 'band')
The draws below stay inside these ranges and needn't reach their ends.
All inputs are finite; a program needn't handle non-finite values.
Results may differ from the reference program's by a relative error of at most 0.0003.
Values may be sent and summed in bfloat16 or wider, within the bound.
A program may use at most 128 MiB of HBM per device.

```python
import jax
import jax.numpy as jnp

NG = 16384
TILE = 512
NFREQ = 2
NDIAG = 1
NBANDS = 16
ROUNDS = 8
N_GBLK = 4


def levels(own_key, dims, pieces, least, high):
    level = 1.0
    for dim, parts in pieces:
        heights = jax.random.uniform(jax.random.fold_in(jax.random.fold_in(own_key, 6), dim), (parts,), jnp.float32, least / len(pieces), high / len(pieces))
        level = level * jnp.repeat(jnp.exp(heights), dims[dim] // parts).reshape((-1,) + (1,) * (len(dims) - 1 - dim))
    return level


def centred(key, shape, deviation, bound, pieces=(), held_as=jnp.bfloat16):
    result = jax.random.normal(key, shape, jnp.float32) * deviation
    if len(pieces) > 0:
        result = levels(key, shape, pieces, -0.22, 0.18) * result
    return jnp.clip(result, min=-bound, max=bound).astype(held_as)


def setup_inputs(seed: int = 0) -> dict:
    arg_keys = jax.random.split(jax.random.key(seed), 3)
    return {
        "eps_inv": centred(arg_keys[0], (NFREQ, 2, ROUNDS, N_GBLK, TILE, NG), 1.0, 6.0, ((3, 4), (5, 8))),
        "pair_elements": centred(arg_keys[1], (2, NDIAG, NBANDS, NG), NG ** -0.5, 0.046875, ((2, 8),)),
    }


def reference(eps_inv, pair_elements):
    matrices = eps_inv.reshape(NFREQ, 2, NG, NG)
    flat = pair_elements.reshape(2 * NDIAG * NBANDS, NG)
    real_part = pair_elements[0].astype(jnp.float32)
    imag_part = pair_elements[1].astype(jnp.float32)
    results = []
    for frequency in range(NFREQ):
        along_a = jnp.dot(flat, matrices[frequency, 0].T, preferred_element_type=jnp.float32).reshape(2, NDIAG, NBANDS, NG)
        along_b = jnp.dot(flat, matrices[frequency, 1].T, preferred_element_type=jnp.float32).reshape(2, NDIAG, NBANDS, NG)
        image_re = along_a[0] - along_b[1]
        image_im = along_a[1] + along_b[0]
        sigma_re = jnp.sum(real_part * image_re + imag_part * image_im, axis=-1)
        sigma_im = jnp.sum(real_part * image_im - imag_part * image_re, axis=-1)
        results.append(jnp.stack([sigma_re, sigma_im]))
    return jnp.stack(results)
```

```python
import functools

import jax
import jax.numpy as jnp
from jax import lax
from jax.experimental import pallas as pl
from jax.experimental.pallas import tpu as pltpu
from jax.sharding import PartitionSpec as P

MESH = pl.DeviceIdType.MESH
RING_BYTES = 40 * 1024 * 1024
LANES = 128


def kernel(
    n, groups, eps, pair, out,
    slots, pairs, rowbuf, colbuf, wide, lhs, cols, swapped, acc, part, got, total, gathered,
    slot_sem, row_local, local_sem, row_send, row_recv, col_send, col_recv, one_send, one_recv, two_send, two_recv,
):
    me = lax.axis_index("band")
    group = lax.axis_index("gblk")
    freqs, rounds, tile_rows, width = eps.shape[0], eps.shape[2], eps.shape[4], eps.shape[5]
    states, bands = pair.shape[1], pair.shape[2]
    own = states * bands
    per_freq = 2 * rounds
    chunks = freqs * per_freq
    ring = slots.shape[0]

    def fetch(index):
        f = index // per_freq
        c = (index // rounds) % 2
        r = index % rounds
        s = index % ring
        return pltpu.make_async_copy(eps.at[f, c, r, 0], slots.at[s], slot_sem.at[s])

    row_copies = []
    for r in range(rounds):
        first = pl.multiple_of((r * groups + group) * tile_rows, tile_rows)
        row_copies.append(
            pltpu.make_async_copy(
                pair.at[:, :, :, pl.ds(first, tile_rows)],
                rowbuf.at[0, :, :, :, pl.ds(r * tile_rows, tile_rows)],
                row_local.at[r],
            )
        )
    for copy in row_copies:
        copy.start()
    pair_copy = pltpu.make_async_copy(pair, pairs, local_sem.at[0])
    pair_copy.start()
    own_first = pl.multiple_of(me * width, width)
    col_copy = pltpu.make_async_copy(pair.at[:, :, :, pl.ds(own_first, width)], colbuf.at[0], local_sem.at[1])
    col_copy.start()
    for index in range(min(ring, chunks)):
        fetch(index).start()

    barrier = pltpu.get_barrier_semaphore()
    for k in range(1, n):
        pl.semaphore_signal(barrier, inc=1, device_id=(lax.rem(me + k, n), group), device_id_type=MESH)
    for k in range(1, groups):
        pl.semaphore_signal(barrier, inc=1, device_id=(me, lax.rem(group + k, groups)), device_id_type=MESH)
    acc[...] = jnp.zeros_like(acc)
    for copy in row_copies:
        copy.wait()
    pair_copy.wait()
    col_copy.wait()
    pl.semaphore_wait(barrier, n + groups - 2)

    row_sends, col_sends = [], []
    for k in range(1, n):
        copy = pltpu.make_async_remote_copy(
            src_ref=rowbuf.at[0], dst_ref=rowbuf.at[k], send_sem=row_send.at[k], recv_sem=row_recv.at[k],
            device_id=(lax.rem(me + k, n), group), device_id_type=MESH,
        )
        copy.start()
        row_sends.append(copy)
    for k in range(1, n):
        target = lax.rem(me + k, n)
        first = pl.multiple_of(target * width, width)
        copy = pltpu.make_async_remote_copy(
            src_ref=pairs.at[:, :, :, pl.ds(first, width)], dst_ref=colbuf.at[k],
            send_sem=col_send.at[k], recv_sem=col_recv.at[k],
            device_id=(target, group), device_id_type=MESH,
        )
        copy.start()
        col_sends.append(copy)

    def place(k):
        for j in range(2):
            for s in range(states):
                at = (2 * k + j) * own + s * bands
                wide[at:at + bands, :] = rowbuf[k, j, s].astype(jnp.float32)

    place(0)
    for k in range(1, n):
        row_sends[k - 1].wait_recv()
        place(k)
    for r in range(rounds):
        lhs[r] = wide[:, r * tile_rows:(r + 1) * tile_rows].astype(jnp.bfloat16)

    def place_columns(k):
        for j in range(2):
            for s in range(states):
                piece = colbuf[k, j, s].astype(jnp.float32)
                at = (2 * k + j) * own + s * bands
                cols[at:at + bands, :] = piece
                other = (2 * k + 1 - j) * own + s * bands
                swapped[other:other + bands, :] = piece if j == 0 else -piece

    one_copies = []
    for f in range(freqs):
        def step(i, carry):
            index = f * per_freq + i
            fetch(index).wait()
            c = i // rounds
            acc[f, c] += jnp.dot(lhs[i % rounds], slots[index % ring], preferred_element_type=jnp.float32)

            @pl.when(index + ring < chunks)
            def _():
                fetch(index + ring).start()

            return carry

        lax.fori_loop(0, per_freq, step, 0)
        if f == 0:
            place_columns(0)
            for k in range(1, n):
                col_sends[k - 1].wait_recv()
                place_columns(k)
        real = jnp.zeros((acc.shape[2], LANES), jnp.float32)
        imag = jnp.zeros((acc.shape[2], LANES), jnp.float32)
        for start in range(0, width, LANES):
            window = slice(start, start + LANES)
            x, y = acc[f, 0, :, window], acc[f, 1, :, window]
            c, d = cols[:, window], swapped[:, window]
            real += x * c + y * d
            imag += y * c - x * d
        for k in range(n):
            part[f, k, 0:2 * own, :] = real[2 * own * k:2 * own * (k + 1), :]
            part[f, k, 2 * own:4 * own, :] = imag[2 * own * k:2 * own * (k + 1), :]
        for k in range(1, n):
            copy = pltpu.make_async_remote_copy(
                src_ref=part.at[f, k], dst_ref=got.at[f, k], send_sem=one_send.at[f, k], recv_sem=one_recv.at[f, k],
                device_id=(lax.rem(me + n - k, n), group), device_id_type=MESH,
            )
            copy.start()
            one_copies.append(copy)

    for f in range(freqs):
        value = part[f, 0]
        for k in range(1, n):
            one_copies[f * (n - 1) + k - 1].wait_recv()
            value += got[f, k]
        total[f] = value
        gathered[group, f] = value
    two_copies = []
    for k in range(1, groups):
        copy = pltpu.make_async_remote_copy(
            src_ref=total, dst_ref=gathered.at[group], send_sem=two_send.at[k], recv_sem=two_recv.at[k],
            device_id=(me, lax.rem(group + k, groups)), device_id_type=MESH,
        )
        copy.start()
        two_copies.append(copy)
    for copy in two_copies:
        copy.wait_recv()
    lane = lax.broadcasted_iota(jnp.int32, (1, bands), 1)
    for f in range(freqs):
        value = gathered[0, f]
        for k in range(1, groups):
            value += gathered[k, f]
        sums = jnp.sum(value, axis=1, keepdims=True)
        for c in range(2):
            for s in range(states):
                row = jnp.zeros((1, bands), jnp.float32)
                for b in range(bands):
                    at = 2 * own * c + s * bands + b
                    row = jnp.where(lane == b, sums[at:at + 1, :] + sums[at + own:at + own + 1, :], row)
                out[f, c, s:s + 1, :] = row
    for copy in row_sends + col_sends + one_copies + two_copies:
        copy.wait_send()


def shards(n, groups, eps_inv, pair_elements):
    freqs, _, rounds, _, tile_rows, width = eps_inv.shape
    _, states, bands, length = pair_elements.shape
    own = states * bands
    rows = 2 * own * n
    ring = max(1, min(freqs * 2 * rounds, RING_BYTES // (tile_rows * width * 2)))
    dma = pltpu.SemaphoreType.DMA
    return pl.pallas_call(
        functools.partial(kernel, n, groups),
        out_shape=jax.ShapeDtypeStruct((freqs, 2, states, bands), jnp.float32),
        in_specs=[pl.BlockSpec(memory_space=pl.ANY)] * 2,
        out_specs=pl.BlockSpec(memory_space=pltpu.VMEM),
        scratch_shapes=[
            pltpu.VMEM((ring, tile_rows, width), jnp.bfloat16),
            pltpu.VMEM((2, states, bands, length), jnp.bfloat16),
            pltpu.VMEM((n, 2, states, bands, rounds * tile_rows), jnp.bfloat16),
            pltpu.VMEM((n, 2, states, bands, width), jnp.bfloat16),
            pltpu.VMEM((rows, rounds * tile_rows), jnp.float32),
            pltpu.VMEM((rounds, rows, tile_rows), jnp.bfloat16),
            pltpu.VMEM((rows, width), jnp.float32),
            pltpu.VMEM((rows, width), jnp.float32),
            pltpu.VMEM((freqs, 2, rows, width), jnp.float32),
            pltpu.VMEM((freqs, n, 4 * own, LANES), jnp.float32),
            pltpu.VMEM((freqs, n, 4 * own, LANES), jnp.float32),
            pltpu.VMEM((freqs, 4 * own, LANES), jnp.float32),
            pltpu.VMEM((groups, freqs, 4 * own, LANES), jnp.float32),
            dma((ring,)), dma((rounds,)), dma((2,)),
            dma((n,)), dma((n,)), dma((n,)), dma((n,)),
            dma((freqs, n)), dma((freqs, n)), dma((groups,)), dma((groups,)),
        ],
        compiler_params=pltpu.CompilerParams(
            collective_id=0, has_side_effects=True, vmem_limit_bytes=60 * 1024 * 1024
        ),
    )(eps_inv, pair_elements)


def solution(mesh):
    placed = (P(None, None, None, "gblk", None, "band"), P(None, None, "band", None))
    return jax.shard_map(
        functools.partial(shards, mesh.shape["band"], mesh.shape["gblk"]),
        mesh=mesh, in_specs=placed, out_specs=P(None, None, None, "band"), check_vma=False,
    )
```

```python
import functools

import jax
import jax.numpy as jnp
from jax import lax
from jax.experimental import pallas as pl
from jax.experimental.pallas import tpu as pltpu
from jax.sharding import PartitionSpec as P

MESH = pl.DeviceIdType.MESH
RING_BYTES = 40 * 1024 * 1024
SPAN = 2
EARLY = 10
LANES = 128


def kernel(
    n, groups, eps, pair, out,
    slots, pairs, rowbuf, colbuf, wide, lhs, cols, swapped, acc, part, got,
    slot_sem, row_local, local_sem, row_send, row_recv, col_send, col_recv, one_send, one_recv,
):
    me = lax.axis_index("band")
    group = lax.axis_index("gblk")
    freqs, rounds, tile_rows, width = eps.shape[0], eps.shape[2], eps.shape[4], eps.shape[5]
    states, bands = pair.shape[1], pair.shape[2]
    own = states * bands
    span = slot_sem.shape[1]
    per_part = rounds // span
    per_freq = 2 * per_part
    chunks = freqs * per_freq
    ring = slots.shape[0]

    def fetch(index):
        f = index // per_freq
        c = (index // per_part) % 2
        r = (index % per_part) * span
        s = index % ring
        return [
            pltpu.make_async_copy(
                eps.at[f, c, r + h, 0], slots.at[s, pl.ds(h * tile_rows, tile_rows)], slot_sem.at[s, h]
            )
            for h in range(span)
        ]

    def begin(index):
        for copy in fetch(index):
            copy.start(priority=1)

    row_copies = []
    for r in range(rounds):
        first = pl.multiple_of((r * groups + group) * tile_rows, tile_rows)
        row_copies.append(
            pltpu.make_async_copy(
                pair.at[:, :, :, pl.ds(first, tile_rows)],
                rowbuf.at[0, :, :, :, pl.ds(r * tile_rows, tile_rows)],
                row_local.at[r],
            )
        )
    for copy in row_copies:
        copy.start()
    pair_copy = pltpu.make_async_copy(pair, pairs, local_sem.at[0])
    pair_copy.start()
    own_first = pl.multiple_of(me * width, width)
    col_copy = pltpu.make_async_copy(pair.at[:, :, :, pl.ds(own_first, width)], colbuf.at[0], local_sem.at[1])
    col_copy.start()
    first_batch = min(EARLY, ring)
    for index in range(first_batch):
        begin(index)

    barrier = pltpu.get_barrier_semaphore()
    others = [(k, g) for g in range(groups) for k in range(n) if (k, g) != (0, 0)]
    for k, g in others:
        there = (lax.rem(me + k, n), lax.rem(group + g, groups))
        pl.semaphore_signal(barrier, inc=1, device_id=there, device_id_type=MESH)
    acc[...] = jnp.zeros_like(acc)
    for copy in row_copies:
        copy.wait()
    pair_copy.wait()
    col_copy.wait()
    pl.semaphore_wait(barrier, len(others))

    row_sends, col_sends = [], []
    for k in range(1, n):
        copy = pltpu.make_async_remote_copy(
            src_ref=rowbuf.at[0], dst_ref=rowbuf.at[k], send_sem=row_send.at[k], recv_sem=row_recv.at[k],
            device_id=(lax.rem(me + k, n), group), device_id_type=MESH,
        )
        copy.start()
        row_sends.append(copy)
    for k in range(1, n):
        target = lax.rem(me + k, n)
        first = pl.multiple_of(target * width, width)
        copy = pltpu.make_async_remote_copy(
            src_ref=pairs.at[:, :, :, pl.ds(first, width)], dst_ref=colbuf.at[k],
            send_sem=col_send.at[k], recv_sem=col_recv.at[k],
            device_id=(target, group), device_id_type=MESH,
        )
        copy.start()
        col_sends.append(copy)
    for index in range(first_batch, ring):
        begin(index)

    def place(k):
        for j in range(2):
            for s in range(states):
                at = (2 * k + j) * own + s * bands
                wide[at:at + bands, :] = rowbuf[k, j, s].astype(jnp.float32)

    place(0)
    for k in range(1, n):
        row_sends[k - 1].wait_recv()
        place(k)
    depth = span * tile_rows
    for r in range(per_part):
        lhs[r] = wide[:, r * depth:(r + 1) * depth].astype(jnp.bfloat16)

    def place_columns(k):
        for j in range(2):
            for s in range(states):
                piece = colbuf[k, j, s].astype(jnp.float32)
                at = (2 * k + j) * own + s * bands
                cols[at:at + bands, :] = piece
                other = (2 * k + 1 - j) * own + s * bands
                swapped[other:other + bands, :] = piece if j == 0 else -piece

    one_copies = []
    for f in range(freqs):
        def step(i, carry):
            index = f * per_freq + i
            for copy in fetch(index):
                copy.wait()
            c = i // per_part
            acc[f, c] += jnp.dot(lhs[i % per_part], slots[index % ring], preferred_element_type=jnp.float32)

            @pl.when(index + ring < chunks)
            def _():
                begin(index + ring)

            return carry

        lax.fori_loop(0, per_freq, step, 0)
        if f == 0:
            place_columns(0)
            for k in range(1, n):
                col_sends[k - 1].wait_recv()
                place_columns(k)
        real = jnp.zeros((acc.shape[2], LANES), jnp.float32)
        imag = jnp.zeros((acc.shape[2], LANES), jnp.float32)
        for start in range(0, width, LANES):
            window = slice(start, start + LANES)
            x, y = acc[f, 0, :, window], acc[f, 1, :, window]
            c, d = cols[:, window], swapped[:, window]
            real += x * c + y * d
            imag += y * c - x * d
        shape = real.shape
        lane = lax.broadcasted_iota(jnp.int32, shape, 1)
        turn = lax.rem(lax.broadcasted_iota(jnp.int32, shape, 0), 2 * own)
        marked = jnp.where(lane == turn, jnp.sum(real, axis=1, keepdims=True), 0.0)
        marked += jnp.where(lane == turn + 2 * own, jnp.sum(imag, axis=1, keepdims=True), 0.0)
        for k in range(n):
            part[f, k] = jnp.sum(marked[2 * own * k:2 * own * (k + 1), :], axis=0, keepdims=True)
        place_of = me * groups + group
        got[f, place_of] = part[f, 0]
        for k, g in others:
            copy = pltpu.make_async_remote_copy(
                src_ref=part.at[f, k], dst_ref=got.at[f, place_of],
                send_sem=one_send.at[f, k * groups + g], recv_sem=one_recv.at[f, k * groups + g],
                device_id=(lax.rem(me + n - k, n), lax.rem(group + g, groups)), device_id_type=MESH,
            )
            copy.start()
            one_copies.append(copy)

    for copy in one_copies:
        copy.wait_recv()
    for f in range(freqs):
        value = got[f, 0]
        for k in range(1, n * groups):
            value += got[f, k]
        for c in range(2):
            for s in range(states):
                at = 2 * own * c + s * bands
                out[f, c, s:s + 1, :] = value[:, at:at + bands] + value[:, at + own:at + own + bands]
    for copy in row_sends + col_sends + one_copies:
        copy.wait_send()


def shards(n, groups, eps_inv, pair_elements):
    freqs, _, rounds, _, tile_rows, width = eps_inv.shape
    _, states, bands, length = pair_elements.shape
    own = states * bands
    rows = 2 * own * n
    span = SPAN if rounds % SPAN == 0 else 1
    depth = span * tile_rows
    ring = max(1, min(freqs * 2 * rounds // span, RING_BYTES // (depth * width * 2)))
    dma = pltpu.SemaphoreType.DMA
    return pl.pallas_call(
        functools.partial(kernel, n, groups),
        out_shape=jax.ShapeDtypeStruct((freqs, 2, states, bands), jnp.float32),
        in_specs=[pl.BlockSpec(memory_space=pl.ANY)] * 2,
        out_specs=pl.BlockSpec(memory_space=pltpu.VMEM),
        scratch_shapes=[
            pltpu.VMEM((ring, depth, width), jnp.bfloat16),
            pltpu.VMEM((2, states, bands, length), jnp.bfloat16),
            pltpu.VMEM((n, 2, states, bands, rounds * tile_rows), jnp.bfloat16),
            pltpu.VMEM((n, 2, states, bands, width), jnp.bfloat16),
            pltpu.VMEM((rows, rounds * tile_rows), jnp.float32),
            pltpu.VMEM((rounds // span, rows, depth), jnp.bfloat16),
            pltpu.VMEM((rows, width), jnp.float32),
            pltpu.VMEM((rows, width), jnp.float32),
            pltpu.VMEM((freqs, 2, rows, width), jnp.float32),
            pltpu.VMEM((freqs, n, 1, LANES), jnp.float32),
            pltpu.VMEM((freqs, n * groups, 1, LANES), jnp.float32),
            dma((ring, span)), dma((rounds,)), dma((2,)),
            dma((n,)), dma((n,)), dma((n,)), dma((n,)),
            dma((freqs, n * groups)), dma((freqs, n * groups)),
        ],
        compiler_params=pltpu.CompilerParams(
            collective_id=0, has_side_effects=True, vmem_limit_bytes=60 * 1024 * 1024
        ),
    )(eps_inv, pair_elements)


def solution(mesh):
    placed = (P(None, None, None, "gblk", None, "band"), P(None, None, "band", None))
    return jax.shard_map(
        functools.partial(shards, mesh.shape["band"], mesh.shape["gblk"]),
        mesh=mesh, in_specs=placed, out_specs=P(None, None, None, "band"), check_vma=False,
    )
```
